32 devices in a mesh: groups: 2 (over x), ctx: 16 (over z, y, core).
Axes of the slice: x: 2, y: 2, z: 4, core: 2. Of those that a mesh axis runs over, the one named last changes fastest.
Arguments:
- query_states: bfloat16 [16384, 32, 128], P(('groups', 'ctx')), parts along dimension 0, may hold values from -20 to 20
- key_states: bfloat16 [16384, 8, 128], P(('groups', 'ctx')), parts along dimension 0, may hold values from -4 to 4
- value_states: bfloat16 [16384, 8, 128], P(('groups', 'ctx')), parts along dimension 0, may hold values from -6 to 6
- vert_blocks: int32 [16, 4], P('groups'), parts along dimension 0, may hold values from 0 to 63, as said below
- vert_count: int32 [16], P('groups'), parts along dimension 0, may hold values from 1 to 4, as said below
- slash_offsets: int32 [16, 4], P('groups'), parts along dimension 0, may hold values from 0 to 8, as said below
- slash_count: int32 [16], P('groups'), parts along dimension 0, may hold values from 1 to 4, as said below
Outputs:
- attended: bfloat16 [16384, 32, 128], P(('groups', 'ctx')), parts along dimension 0
The draws below stay inside these ranges and needn't reach their ends.
There are 2 independent parts, one for each index of `groups`. The reference program is written for one: setup_inputs(seed, part) draws one part's arguments, and reference() takes and returns one part's arrays. A program takes and returns all parts, laid end to end along the dimension named above; each array names one. Nothing has to cross between parts.
Inputs may be any that keep to these rules, and one draw needn't show every extreme that they name: `vert_blocks`: the 4 entries of each head are distinct; in some head the first entry lies in one of the first 4 blocks. `vert_count`: some head uses all 4 entries. `slash_offsets`: the 4 entries of each head are distinct and the first is 0. `slash_count`: some head uses all 4 entries.
All inputs are finite; a program needn't handle non-finite values.
Results may differ from the reference program's by a relative error of at most 0.0048.
Values may be sent and summed in bfloat16 or wider, within the bound.
A program may use at most 128 MiB of HBM per device.

```python
import math
import jax
import jax.numpy as jnp
from jax import lax

QH = 32
KVH = 8
DH = 128
BLOCK = 128
NV = 4
NS = 4
SEQ_DEV = 512
TOKENS = 8192
NBLK = 64


def draw_query_states(key, part):
    base = jnp.clip(jax.random.normal(jax.random.fold_in(key, 11), (TOKENS, QH, DH), jnp.float32), -4.0, 4.0)
    return base.astype(jnp.bfloat16)


def draw_key_states(key, part):
    base = jnp.clip(jax.random.normal(jax.random.fold_in(key, 12), (TOKENS, KVH, DH), jnp.float32), -4.0, 4.0)
    return base.astype(jnp.bfloat16)


def draw_vert_blocks(key, part):
    head_keys = jax.random.split(jax.random.fold_in(key, 21), KVH)
    picked = jax.vmap(lambda one_key: jax.random.permutation(one_key, NBLK)[:NV])(head_keys).astype(jnp.int32)
    first_dev = SEQ_DEV // BLOCK
    lowest = jax.random.randint(jax.random.fold_in(key, 22), (), 0, first_dev).astype(jnp.int32)
    others = jax.random.permutation(jax.random.fold_in(key, 23), NBLK - 1)[:NV - 1].astype(jnp.int32)
    others = others + (others >= lowest).astype(jnp.int32)
    special = jnp.concatenate((lowest[None], others))
    chosen = jax.random.randint(jax.random.fold_in(key, 24), (), 0, KVH)
    picked = jnp.where((jnp.arange(KVH) == chosen)[:, None], special[None, :], picked)
    return picked.astype(jnp.int32)


def draw_vert_count(key, part):
    counts = jax.random.randint(jax.random.fold_in(key, 31), (KVH,), 1, NV + 1)
    fullest = jax.random.randint(jax.random.fold_in(key, 32), (), 0, KVH)
    return counts.at[fullest].set(NV).astype(jnp.int32)


def draw_slash_offsets(key, part):
    head_keys = jax.random.split(jax.random.fold_in(key, 41), KVH)
    reach = 2 * (SEQ_DEV // BLOCK)
    others = jax.vmap(lambda one_key: jax.random.permutation(one_key, reach)[:NS - 1] + 1)(head_keys)
    return jnp.concatenate((jnp.zeros((KVH, 1), jnp.int32), others.astype(jnp.int32)), axis=1)


def draw_slash_count(key, part):
    counts = jax.random.randint(jax.random.fold_in(key, 51), (KVH,), 1, NS + 1)
    fullest = jax.random.randint(jax.random.fold_in(key, 52), (), 0, KVH)
    return counts.at[fullest].set(NS).astype(jnp.int32)


def block_scale(rng, shape, cuts, low, largest):
    def one(position, blocks):
        draws = jax.random.uniform(jax.random.fold_in(jax.random.fold_in(rng, 6), position), (blocks,), jnp.float32, low / len(cuts), largest / len(cuts))
        return jnp.repeat(jnp.exp(draws), shape[position] // blocks).reshape((-1,) + (1,) * (len(shape) - position - 1))

    gain = one(*cuts[0])
    for cut in cuts[1:]:
        gain = gain * one(*cut)
    return gain


def centred(key, dims, deviation, bound, pieces=(), kind=jnp.bfloat16):
    entries = deviation * jax.random.normal(key, dims, jnp.float32)
    if pieces:
        entries = entries * block_scale(key, dims, pieces, -0.22, 0.18)
    return jnp.clip(entries, -bound, bound).astype(kind)


def setup_inputs(seed: int = 0, part: int = 0) -> dict:
    key_of = jax.random.split(jax.random.key(seed), 8)
    part_keys = jax.random.split(jax.random.fold_in(key_of[7], part), 8)
    query_states = draw_query_states(jax.random.fold_in(jax.random.fold_in(key_of[7], part), 71), part)
    key_states = draw_key_states(jax.random.fold_in(jax.random.fold_in(key_of[7], part), 71), part)
    value_states = centred(part_keys[2], (TOKENS, KVH, DH), 1.0, 6.0, ((0, 16),))
    vert_blocks = draw_vert_blocks(jax.random.fold_in(jax.random.fold_in(key_of[7], part), 71), part)
    vert_count = draw_vert_count(jax.random.fold_in(jax.random.fold_in(key_of[7], part), 71), part)
    slash_offsets = draw_slash_offsets(jax.random.fold_in(jax.random.fold_in(key_of[7], part), 71), part)
    slash_count = draw_slash_count(jax.random.fold_in(jax.random.fold_in(key_of[7], part), 71), part)
    return dict(query_states=query_states, key_states=key_states, value_states=value_states, vert_blocks=vert_blocks, vert_count=vert_count, slash_offsets=slash_offsets, slash_count=slash_count)


def reference(query_states, key_states, value_states, vert_blocks, vert_count, slash_offsets, slash_count):
    group_size = QH // KVH
    key_tiles_all = key_states.reshape(NBLK, BLOCK, KVH, DH)
    value_tiles_all = value_states.reshape(NBLK, BLOCK, KVH, DH)
    head_ids = jnp.arange(KVH, dtype=jnp.int32)
    vert_slot = jnp.arange(NV, dtype=jnp.int32)[None, :] < vert_count[:, None]
    slash_slot = jnp.arange(NS, dtype=jnp.int32)[None, :] < slash_count[:, None]
    inv_root = 1.0 / math.sqrt(DH)
    within = jnp.arange(BLOCK, dtype=jnp.int32)

    def query_block(qblock):
        slash_blocks = qblock - slash_offsets
        repeated = jnp.any(vert_slot[:, None, :] & (vert_blocks[:, None, :] == slash_blocks[:, :, None]), axis=-1)
        slash_ok = slash_slot & (slash_blocks >= 0) & jnp.logical_not(repeated)
        vert_ok = vert_slot & (vert_blocks <= qblock)
        key_blocks = jnp.concatenate((vert_blocks, slash_blocks), axis=1)
        usable = jnp.concatenate((vert_ok, slash_ok), axis=1)
        clipped = jnp.clip(key_blocks, 0, NBLK - 1)
        key_tiles = key_tiles_all[clipped, :, head_ids[:, None], :]
        value_tiles = value_tiles_all[clipped, :, head_ids[:, None], :]
        query_rows = lax.dynamic_slice_in_dim(query_states, qblock * BLOCK, BLOCK, 0).reshape(BLOCK, KVH, group_size, DH)
        scores = jnp.einsum('qgrd,gntd->grqnt', query_rows.astype(jnp.float32), key_tiles.astype(jnp.float32)) * inv_root
        scores = scores.reshape(KVH, group_size, BLOCK, (NV + NS) * BLOCK)
        key_pos = (key_blocks[:, :, None] * BLOCK + within[None, None, :]).reshape(KVH, (NV + NS) * BLOCK)
        query_pos = qblock * BLOCK + within
        allowed = jnp.repeat(usable, BLOCK, axis=1)[:, None, :] & (key_pos[:, None, :] <= query_pos[None, :, None])
        allowed = allowed[:, None, :, :]
        masked = jnp.where(allowed, scores, -1e+30)
        row_max = lax.optimization_barrier(jnp.max(masked, axis=-1, keepdims=True))
        powers = jnp.where(allowed, jnp.exp(masked - row_max), 0.0)
        weights = (powers / lax.optimization_barrier(jnp.sum(powers, axis=-1, keepdims=True))).astype(jnp.bfloat16)
        values_flat = value_tiles.reshape(KVH, (NV + NS) * BLOCK, DH).astype(jnp.float32)
        result = jnp.einsum('grqk,gkd->qgrd', weights.astype(jnp.float32), values_flat)
        return result.reshape(BLOCK, QH, DH).astype(jnp.bfloat16)
    blocks = lax.map(query_block, jnp.arange(NBLK, dtype=jnp.int32))
    return blocks.reshape(TOKENS, QH, DH)
```

```python
import functools
import math

import jax
import jax.numpy as jnp
from jax import lax
from jax.experimental import pallas as pl
from jax.experimental.pallas import tpu as pltpu
from jax.sharding import PartitionSpec as P

BLOCK = 128
REACH = 2


def attend_kernel(
    dims, vb_ref, vc_ref, so_ref, sc_ref, dev_ref, q_ref, kv_ref, out_ref, list_ref
):
    per_dev, n_vert, n_slash, group_size, head_dim = dims
    n_window = (REACH + 1) * per_dev
    head = pl.program_id(0)
    device = dev_ref[0]
    scale = math.log2(math.e) / math.sqrt(head_dim)
    rows = group_size * BLOCK
    in_tile = lax.broadcasted_iota(jnp.int32, (rows, BLOCK), 0) % BLOCK
    causal = lax.broadcasted_iota(jnp.int32, (rows, BLOCK), 1) <= in_tile

    def one_block(block, carry):
        qblock = device * per_dev + block
        count = jnp.int32(0)
        for v in range(n_vert):
            list_ref[count] = n_window + v
            ok = (v < vc_ref[head]) & (vb_ref[head, v] < qblock)
            count = count + ok.astype(jnp.int32)
        for s in range(1, n_slash):
            offset = so_ref[head, s]
            ok = (s < sc_ref[head]) & (offset <= qblock)
            for v in range(n_vert):
                ok = ok & ((v >= vc_ref[head]) | (vb_ref[head, v] != qblock - offset))
            list_ref[count] = REACH * per_dev + block - offset
            count = count + ok.astype(jnp.int32)

        start = pl.multiple_of(block * BLOCK, BLOCK)
        for n in range(n_vert + n_slash):

            @pl.when(count == n)
            def _(n=n):
                queries = jnp.concatenate(
                    [
                        q_ref[pl.ds(start, BLOCK), h * head_dim : (h + 1) * head_dim]
                        for h in range(group_size)
                    ],
                    axis=0,
                )
                spots = [REACH * per_dev + block] + [list_ref[i] for i in range(n)]
                scores = []
                for i, spot in enumerate(spots):
                    tile = lax.dot_general(
                        queries,
                        kv_ref[0, spot, 0],
                        (((1,), (1,)), ((), ())),
                        preferred_element_type=jnp.float32,
                    )
                    scores.append(jnp.where(causal, tile, -1e30) if i == 0 else tile)
                top = functools.reduce(jnp.maximum, scores)
                top = jnp.max(top, axis=1, keepdims=True) * scale
                powers = [jnp.exp2(tile * scale - top) for tile in scores]
                total = jnp.sum(functools.reduce(jnp.add, powers), axis=1, keepdims=True)
                weights = jnp.concatenate([p.astype(jnp.bfloat16) for p in powers], axis=1)
                values = jnp.concatenate([kv_ref[0, spot, 1] for spot in spots], axis=0)
                result = jnp.dot(weights, values, preferred_element_type=jnp.float32)
                result = (result / total).astype(jnp.bfloat16)
                for h in range(group_size):
                    out_ref[pl.ds(start, BLOCK), h * head_dim : (h + 1) * head_dim] = result[
                        h * BLOCK : (h + 1) * BLOCK
                    ]

        return carry

    lax.fori_loop(0, per_dev, one_block, 0)


def attend(queries, tiles, vert_blocks, vert_count, slash_offsets, slash_count, device, group_size):
    rows_dev = queries.shape[0]
    kv_heads, n_tiles, _, _, head_dim = tiles.shape
    n_vert = vert_blocks.shape[1]
    n_slash = slash_offsets.shape[1]
    per_dev = rows_dev // BLOCK
    width = group_size * head_dim
    dims = (per_dev, n_vert, n_slash, group_size, head_dim)
    pairs = kv_heads * group_size * rows_dev * (n_vert + n_slash) * BLOCK
    return pl.pallas_call(
        functools.partial(attend_kernel, dims),
        out_shape=jax.ShapeDtypeStruct(queries.shape, jnp.bfloat16),
        grid_spec=pltpu.PrefetchScalarGridSpec(
            num_scalar_prefetch=5,
            grid=(kv_heads,),
            in_specs=[
                pl.BlockSpec((rows_dev, width), lambda g, *_: (0, g)),
                pl.BlockSpec((1, n_tiles, 2, BLOCK, head_dim), lambda g, *_: (g, 0, 0, 0, 0)),
            ],
            out_specs=pl.BlockSpec((rows_dev, width), lambda g, *_: (0, g)),
            scratch_shapes=[pltpu.SMEM((n_vert + n_slash,), jnp.int32)],
        ),
        compiler_params=pltpu.CompilerParams(
            dimension_semantics=("arbitrary",), vmem_limit_bytes=48 * 1024 * 1024
        ),
        cost_estimate=pl.CostEstimate(
            flops=4 * pairs * head_dim, bytes_accessed=4 * queries.size, transcendentals=pairs
        ),
        name="attend",
    )(vert_blocks, vert_count, slash_offsets, slash_count, device, queries, tiles)


def shifted(x, axis, by):
    size = lax.axis_size(axis)
    pairs = [(i, i + by) for i in range(size) if 0 <= i + by < size]
    return lax.ppermute(x, axis, pairs)


def local(
    query_states, key_states, value_states, vert_blocks, vert_count, slash_offsets, slash_count
):
    rows_dev, q_heads, head_dim = query_states.shape
    kv_heads = key_states.shape[1]
    group_size = q_heads // kv_heads
    per_dev = rows_dev // BLOCK
    n_vert = vert_blocks.shape[1]
    device = lax.axis_index("ctx")

    def by_tile(x):
        return jnp.transpose(x.reshape(per_dev, BLOCK, kv_heads, head_dim), (2, 0, 1, 3))

    own = jnp.stack((by_tile(key_states), by_tile(value_states)), axis=2)
    nearby = shifted(own, "ctx", 1)
    farther = shifted(own, "ctx", 2)

    local_block = vert_blocks - device * per_dev
    used_slot = jnp.arange(n_vert)[None, :] < vert_count[:, None]
    mine = used_slot & (local_block >= 0) & (local_block < per_dev)
    term = jnp.take_along_axis(
        own, jnp.clip(local_block, 0, per_dev - 1)[:, :, None, None, None], axis=1
    )
    term = jnp.where(mine[:, :, None, None, None], term, jnp.bfloat16(0))
    columns = lax.psum(term, "ctx")
    tiles = jnp.concatenate((farther, nearby, own, columns), axis=1)
    out = attend(
        query_states.reshape(rows_dev, q_heads * head_dim),
        tiles,
        vert_blocks,
        vert_count,
        slash_offsets,
        slash_count,
        device.reshape(1).astype(jnp.int32),
        group_size,
    )
    return out.reshape(rows_dev, q_heads, head_dim)


def solution(mesh):
    in_specs = (
        P(("groups", "ctx"), None, None),
        P(("groups", "ctx"), None, None),
        P(("groups", "ctx"), None, None),
        P("groups", None),
        P("groups"),
        P("groups", None),
        P("groups"),
    )
    out_specs = P(("groups", "ctx"), None, None)
    return jax.shard_map(local, mesh=mesh, in_specs=in_specs, out_specs=out_specs, check_vma=False)
```

```python
import functools
import math

import jax
import jax.numpy as jnp
from jax import lax
from jax.experimental import pallas as pl
from jax.experimental.pallas import tpu as pltpu
from jax.sharding import PartitionSpec as P

BLOCK = 128
REACH = 2


def attend_kernel(
    dims, vb_ref, vc_ref, so_ref, sc_ref, dev_ref, q_ref, kv_ref, out_ref, list_ref
):
    per_dev, n_vert, n_slash, group_size, head_dim = dims
    n_window = (REACH + 1) * per_dev
    head = pl.program_id(0)
    device = dev_ref[0]
    scale = math.log2(math.e) / math.sqrt(head_dim)
    rows = group_size * BLOCK
    in_tile = lax.broadcasted_iota(jnp.int32, (rows, BLOCK), 0) % BLOCK
    causal = lax.broadcasted_iota(jnp.int32, (rows, BLOCK), 1) <= in_tile

    def one_block(block, carry):
        qblock = device * per_dev + block
        count = jnp.int32(0)
        for v in range(n_vert):
            list_ref[count] = n_window + v
            ok = (v < vc_ref[head]) & (vb_ref[head, v] < qblock)
            count = count + ok.astype(jnp.int32)
        for s in range(1, n_slash):
            offset = so_ref[head, s]
            ok = (s < sc_ref[head]) & (offset <= qblock)
            for v in range(n_vert):
                ok = ok & ((v >= vc_ref[head]) | (vb_ref[head, v] != qblock - offset))
            list_ref[count] = REACH * per_dev + block - offset
            count = count + ok.astype(jnp.int32)

        start = pl.multiple_of(block * BLOCK, BLOCK)
        for n in range(n_vert + n_slash):

            @pl.when(count == n)
            def _(n=n):
                queries = jnp.concatenate(
                    [
                        q_ref[pl.ds(start, BLOCK), h * head_dim : (h + 1) * head_dim]
                        for h in range(group_size)
                    ],
                    axis=0,
                )
                spots = [REACH * per_dev + block] + [list_ref[i] for i in range(n)]
                scores = []
                for i, spot in enumerate(spots):
                    tile = lax.dot_general(
                        queries,
                        kv_ref[0, spot, 0],
                        (((1,), (1,)), ((), ())),
                        preferred_element_type=jnp.float32,
                    )
                    scores.append(jnp.where(causal, tile, -1e30) if i == 0 else tile)
                top = functools.reduce(jnp.maximum, scores)
                top = jnp.max(top, axis=1, keepdims=True) * scale
                powers = [jnp.exp2(tile * scale - top) for tile in scores]
                total = jnp.sum(functools.reduce(jnp.add, powers), axis=1, keepdims=True)
                weights = jnp.concatenate([p.astype(jnp.bfloat16) for p in powers], axis=1)
                values = jnp.concatenate([kv_ref[0, spot, 1] for spot in spots], axis=0)
                result = jnp.dot(weights, values, preferred_element_type=jnp.float32)
                result = (result / total).astype(jnp.bfloat16)
                for h in range(group_size):
                    out_ref[pl.ds(start, BLOCK), h * head_dim : (h + 1) * head_dim] = result[
                        h * BLOCK : (h + 1) * BLOCK
                    ]

        return carry

    lax.fori_loop(0, per_dev, one_block, 0)


def attend(queries, tiles, vert_blocks, vert_count, slash_offsets, slash_count, device, group_size):
    rows_dev = queries.shape[0]
    kv_heads, n_tiles, _, _, head_dim = tiles.shape
    n_vert = vert_blocks.shape[1]
    n_slash = slash_offsets.shape[1]
    per_dev = rows_dev // BLOCK
    width = group_size * head_dim
    dims = (per_dev, n_vert, n_slash, group_size, head_dim)
    pairs = kv_heads * group_size * rows_dev * (n_vert + n_slash) * BLOCK
    return pl.pallas_call(
        functools.partial(attend_kernel, dims),
        out_shape=jax.ShapeDtypeStruct(queries.shape, jnp.bfloat16),
        grid_spec=pltpu.PrefetchScalarGridSpec(
            num_scalar_prefetch=5,
            grid=(kv_heads,),
            in_specs=[
                pl.BlockSpec((rows_dev, width), lambda g, *_: (0, g)),
                pl.BlockSpec((1, n_tiles, 2, BLOCK, head_dim), lambda g, *_: (g, 0, 0, 0, 0)),
            ],
            out_specs=pl.BlockSpec((rows_dev, width), lambda g, *_: (0, g)),
            scratch_shapes=[pltpu.SMEM((n_vert + n_slash,), jnp.int32)],
        ),
        compiler_params=pltpu.CompilerParams(
            dimension_semantics=("arbitrary",), vmem_limit_bytes=48 * 1024 * 1024
        ),
        cost_estimate=pl.CostEstimate(
            flops=4 * pairs * head_dim, bytes_accessed=4 * queries.size, transcendentals=pairs
        ),
        name="attend",
    )(vert_blocks, vert_count, slash_offsets, slash_count, device, queries, tiles)


def spread_kernel(
    dims, own_ref, term_ref, out_ref, acc, landed, full,
    far_send, far_recv, near_send, near_recv, fold_send, fold_recv, grow_send, grow_recv, keep_sem,
):
    size, kv_heads, own_rows, col_rows = dims
    head_rows = (REACH + 1) * own_rows + col_rows
    rounds = size.bit_length() - 1
    device = lax.axis_index("ctx")
    odd = lax.rem(device, 2)
    sends_far = device < size - REACH
    gets_far = device >= REACH
    gets_near = device >= 1
    partners = []
    bits = []
    for k in range(rounds):
        bit = lax.rem(device // (1 << k), 2)
        bits.append(bit)
        partners.append(device + (1 << k) * (1 - 2 * bit))

    def remote(src, dst, send, recv, target):
        return pltpu.make_async_remote_copy(
            src_ref=src, dst_ref=dst, send_sem=send, recv_sem=recv,
            device_id={"ctx": target}, device_id_type=pl.DeviceIdType.MESH,
        )

    def out_rows(head, place, rows):
        return out_ref.at[pl.ds(head * head_rows + place * own_rows, rows)]

    def far_copy(head):
        src = own_ref.at[pl.ds(head * own_rows, own_rows)]
        target = jnp.minimum(device + REACH, size - 1)
        return remote(src, out_rows(head, 0, own_rows), far_send.at[head], far_recv.at[head], target)

    def near_copy(head):
        src = own_ref.at[pl.ds(head * own_rows, own_rows)]
        return remote(
            src, out_rows(head, 1, own_rows), near_send.at[head], near_recv.at[head], partners[0]
        )

    def relay_copy(head):
        return remote(
            out_rows(head, 0, own_rows), out_rows(head, 1, own_rows),
            near_send.at[head], near_recv.at[head], partners[0],
        )

    barrier = pltpu.get_barrier_semaphore()
    for partner in partners:
        pl.semaphore_signal(
            barrier, inc=1, device_id={"ctx": partner}, device_id_type=pl.DeviceIdType.MESH
        )

    @pl.when(sends_far)
    def _():
        pl.semaphore_signal(
            barrier, inc=1, device_id={"ctx": device + REACH}, device_id_type=pl.DeviceIdType.MESH
        )

    @pl.when(gets_far)
    def _():
        pl.semaphore_signal(
            barrier, inc=1, device_id={"ctx": device - REACH}, device_id_type=pl.DeviceIdType.MESH
        )

    arrivals = rounds + sends_far.astype(jnp.int32) + gets_far.astype(jnp.int32)
    pl.semaphore_wait(barrier, arrivals)

    def start_far(heads):
        @pl.when(sends_far)
        def _():
            for head in heads:
                far_copy(head).start()

    early = range(kv_heads // 2)
    late = range(kv_heads // 2, kv_heads)
    base = jnp.int32(0)
    length = kv_heads * col_rows
    offset = 0
    bases = []
    folds = []
    for k in range(rounds):
        half = length // 2
        kept = pl.multiple_of(base + bits[k] * half, 16)
        given = pl.multiple_of(base + (1 - bits[k]) * half, 16)
        source = term_ref if k == 0 else acc
        copy = remote(
            source.at[pl.ds(given, half)], landed.at[pl.ds(offset, half)],
            fold_send.at[k], fold_recv.at[k], partners[k],
        )
        copy.start()
        folds.append(copy)
        if k == min(1, rounds - 1):
            start_far(early)
            for head in range(kv_heads):
                pltpu.make_async_copy(
                    own_ref.at[pl.ds(head * own_rows, own_rows)],
                    out_rows(head, REACH, own_rows), keep_sem.at[head],
                ).start()

            @pl.when(odd == 0)
            def _():
                for head in range(kv_heads):
                    near_copy(head).start()

        copy.wait_recv()
        step = min(half, 256)

        def add(i, carry, kept=kept, offset=offset, source=source, step=step, k=k):
            here = pl.ds(pl.multiple_of(kept + i * step, 16), step)
            there = pl.ds(pl.multiple_of(offset + i * step, 16), step)
            total = source[here, :] + landed[there, :]
            if k == rounds - 1:
                full[here, :] = total
            else:
                acc[here, :] = total
            return carry

        lax.fori_loop(0, half // step, add, 0)
        bases.append(kept)
        base, length, offset = kept, half, offset + half

    grows = []
    for k in reversed(range(rounds)):
        part = pl.ds(bases[k], (kv_heads * col_rows) >> (k + 1))
        copy = remote(full.at[part], full.at[part], grow_send.at[k], grow_recv.at[k], partners[k])
        copy.start()
        grows.append(copy)
        if k == min(1, rounds - 1):
            start_far(late)
        copy.wait_recv()

    cols = []
    for head in range(kv_heads):
        copy = pltpu.make_async_copy(
            full.at[pl.ds(head * col_rows, col_rows)],
            out_rows(head, REACH + 1, col_rows), keep_sem.at[kv_heads + head],
        )
        copy.start()
        cols.append(copy)

    @pl.when(gets_far)
    def _():
        for head in range(kv_heads):
            far_copy(head).wait_recv()

            @pl.when(odd == 1)
            def _(head=head):
                relay_copy(head).start()

    @pl.when((odd == 1) | gets_far)
    def _():
        for head in range(kv_heads):
            near_copy(head).wait_recv()

    @pl.when((odd == 0) | gets_far)
    def _():
        for head in range(kv_heads):
            near_copy(head).wait_send()

    @pl.when(sends_far)
    def _():
        for head in range(kv_heads):
            far_copy(head).wait_send()

    for copy in folds + grows:
        copy.wait_send()
    for head in range(kv_heads):
        pltpu.make_async_copy(
            own_ref.at[pl.ds(head * own_rows, own_rows)],
            out_rows(head, REACH, own_rows), keep_sem.at[head],
        ).wait()
    for copy in cols:
        copy.wait()


def spread(own, term):
    size = lax.axis_size("ctx")
    kv_heads, per_dev, _, _, head_dim = own.shape
    n_vert = term.shape[1]
    own_rows = per_dev * 2 * BLOCK
    col_rows = n_vert * 2 * BLOCK
    n_tiles = (REACH + 1) * per_dev + n_vert
    dims = (size, kv_heads, own_rows, col_rows)
    rounds = size.bit_length() - 1
    dma = pltpu.SemaphoreType.DMA
    columns = pltpu.VMEM((kv_heads * col_rows, head_dim), own.dtype)
    out = pl.pallas_call(
        functools.partial(spread_kernel, dims),
        out_shape=jax.ShapeDtypeStruct((kv_heads * n_tiles * 2 * BLOCK, head_dim), own.dtype),
        in_specs=[pl.BlockSpec(memory_space=pltpu.VMEM)] * 2,
        out_specs=pl.BlockSpec(memory_space=pl.ANY),
        scratch_shapes=[columns, columns, columns]
        + [dma((kv_heads,))] * 4
        + [dma((rounds,))] * 4
        + [dma((2 * kv_heads,))],
        compiler_params=pltpu.CompilerParams(
            collective_id=0, has_side_effects=True, vmem_limit_bytes=48 * 1024 * 1024
        ),
        name="spread",
    )(own.reshape(-1, head_dim), term.reshape(-1, head_dim))
    return out.reshape(kv_heads, n_tiles, 2, BLOCK, head_dim)


def local(
    query_states, key_states, value_states, vert_blocks, vert_count, slash_offsets, slash_count
):
    rows_dev, q_heads, head_dim = query_states.shape
    kv_heads = key_states.shape[1]
    group_size = q_heads // kv_heads
    per_dev = rows_dev // BLOCK
    n_vert = vert_blocks.shape[1]
    device = lax.axis_index("ctx")

    def by_tile(x):
        return jnp.transpose(x.reshape(per_dev, BLOCK, kv_heads, head_dim), (2, 0, 1, 3))

    own = jnp.stack((by_tile(key_states), by_tile(value_states)), axis=2)
    local_block = vert_blocks - device * per_dev
    used_slot = jnp.arange(n_vert)[None, :] < vert_count[:, None]
    mine = used_slot & (local_block >= 0) & (local_block < per_dev)
    term = jnp.take_along_axis(
        own, jnp.clip(local_block, 0, per_dev - 1)[:, :, None, None, None], axis=1
    )
    term = jnp.where(mine[:, :, None, None, None], term, jnp.bfloat16(0))
    tiles = spread(own, term)
    out = attend(
        query_states.reshape(rows_dev, q_heads * head_dim),
        tiles,
        vert_blocks,
        vert_count,
        slash_offsets,
        slash_count,
        device.reshape(1).astype(jnp.int32),
        group_size,
    )
    return out.reshape(rows_dev, q_heads, head_dim)


def solution(mesh):
    in_specs = (
        P(("groups", "ctx"), None, None),
        P(("groups", "ctx"), None, None),
        P(("groups", "ctx"), None, None),
        P("groups", None),
        P("groups"),
        P("groups", None),
        P("groups"),
    )
    out_specs = P(("groups", "ctx"), None, None)
    return jax.shard_map(local, mesh=mesh, in_specs=in_specs, out_specs=out_specs, check_vma=False)
```

```python
import functools
import math

import jax
import jax.numpy as jnp
from jax import lax
from jax.experimental import pallas as pl
from jax.experimental.pallas import tpu as pltpu
from jax.sharding import PartitionSpec as P

BLOCK = 128
REACH = 2


def attend_kernel(
    dims, vb_ref, vc_ref, so_ref, sc_ref, dev_ref, q_ref, kv_ref, out_ref, list_ref
):
    per_dev, n_vert, n_slash, group_size, head_dim = dims
    n_window = (REACH + 1) * per_dev
    head = pl.program_id(0)
    device = dev_ref[0]
    scale = math.log2(math.e) / math.sqrt(head_dim)
    rows = group_size * BLOCK
    in_tile = lax.broadcasted_iota(jnp.int32, (rows, BLOCK), 0) % BLOCK
    causal = lax.broadcasted_iota(jnp.int32, (rows, BLOCK), 1) <= in_tile

    def one_block(block, carry):
        qblock = device * per_dev + block
        count = jnp.int32(0)
        for v in range(n_vert):
            list_ref[count] = n_window + v
            ok = (v < vc_ref[head]) & (vb_ref[head, v] < qblock)
            count = count + ok.astype(jnp.int32)
        for s in range(1, n_slash):
            offset = so_ref[head, s]
            ok = (s < sc_ref[head]) & (offset <= qblock)
            for v in range(n_vert):
                ok = ok & ((v >= vc_ref[head]) | (vb_ref[head, v] != qblock - offset))
            list_ref[count] = REACH * per_dev + block - offset
            count = count + ok.astype(jnp.int32)

        start = pl.multiple_of(block * BLOCK, BLOCK)
        for n in range(n_vert + n_slash):

            @pl.when(count == n)
            def _(n=n):
                queries = jnp.concatenate(
                    [
                        q_ref[pl.ds(start, BLOCK), h * head_dim : (h + 1) * head_dim]
                        for h in range(group_size)
                    ],
                    axis=0,
                )
                spots = [REACH * per_dev + block] + [list_ref[i] for i in range(n)]
                scores = []
                for i, spot in enumerate(spots):
                    tile = lax.dot_general(
                        queries,
                        kv_ref[0, spot, 0],
                        (((1,), (1,)), ((), ())),
                        preferred_element_type=jnp.float32,
                    )
                    scores.append(jnp.where(causal, tile, -1e30) if i == 0 else tile)
                top = functools.reduce(jnp.maximum, scores)
                top = jnp.max(top, axis=1, keepdims=True) * scale
                powers = [jnp.exp2(tile * scale - top) for tile in scores]
                total = jnp.sum(functools.reduce(jnp.add, powers), axis=1, keepdims=True)
                weights = jnp.concatenate([p.astype(jnp.bfloat16) for p in powers], axis=1)
                values = jnp.concatenate([kv_ref[0, spot, 1] for spot in spots], axis=0)
                result = jnp.dot(weights, values, preferred_element_type=jnp.float32)
                result = (result / total).astype(jnp.bfloat16)
                for h in range(group_size):
                    out_ref[pl.ds(start, BLOCK), h * head_dim : (h + 1) * head_dim] = result[
                        h * BLOCK : (h + 1) * BLOCK
                    ]

        return carry

    lax.fori_loop(0, per_dev, one_block, 0)


def attend(queries, tiles, vert_blocks, vert_count, slash_offsets, slash_count, device, group_size):
    rows_dev = queries.shape[0]
    kv_heads, n_tiles, _, _, head_dim = tiles.shape
    n_vert = vert_blocks.shape[1]
    n_slash = slash_offsets.shape[1]
    per_dev = rows_dev // BLOCK
    width = group_size * head_dim
    dims = (per_dev, n_vert, n_slash, group_size, head_dim)
    pairs = kv_heads * group_size * rows_dev * (n_vert + n_slash) * BLOCK
    return pl.pallas_call(
        functools.partial(attend_kernel, dims),
        out_shape=jax.ShapeDtypeStruct(queries.shape, jnp.bfloat16),
        grid_spec=pltpu.PrefetchScalarGridSpec(
            num_scalar_prefetch=5,
            grid=(kv_heads,),
            in_specs=[
                pl.BlockSpec((rows_dev, width), lambda g, *_: (0, g)),
                pl.BlockSpec((1, n_tiles, 2, BLOCK, head_dim), lambda g, *_: (g, 0, 0, 0, 0)),
            ],
            out_specs=pl.BlockSpec((rows_dev, width), lambda g, *_: (0, g)),
            scratch_shapes=[pltpu.SMEM((n_vert + n_slash,), jnp.int32)],
        ),
        compiler_params=pltpu.CompilerParams(
            dimension_semantics=("arbitrary",), vmem_limit_bytes=48 * 1024 * 1024
        ),
        cost_estimate=pl.CostEstimate(
            flops=4 * pairs * head_dim, bytes_accessed=4 * queries.size, transcendentals=pairs
        ),
        name="attend",
    )(vert_blocks, vert_count, slash_offsets, slash_count, device, queries, tiles)


def spread_kernel(
    dims, own_ref, term_ref, out_ref, acc, landed, full,
    far_send, far_recv, near_send, near_recv, fold_send, fold_recv, grow_send, grow_recv, keep_sem,
):
    size, kv_heads, own_rows, col_rows = dims
    head_rows = (REACH + 1) * own_rows + col_rows
    rounds = size.bit_length() - 1
    device = lax.axis_index("ctx")
    odd = lax.rem(device, 2)
    sends_far = device < size - REACH
    gets_far = device >= REACH
    gets_near = device >= 1
    partners = []
    bits = []
    for k in range(rounds):
        bit = lax.rem(device // (1 << k), 2)
        bits.append(bit)
        partners.append(device + (1 << k) * (1 - 2 * bit))

    def remote(src, dst, send, recv, target):
        return pltpu.make_async_remote_copy(
            src_ref=src, dst_ref=dst, send_sem=send, recv_sem=recv,
            device_id={"ctx": target}, device_id_type=pl.DeviceIdType.MESH,
        )

    def out_rows(head, place, rows):
        return out_ref.at[pl.ds(head * head_rows + place * own_rows, rows)]

    def far_copy(head):
        src = own_ref.at[pl.ds(head * own_rows, own_rows)]
        target = jnp.minimum(device + REACH, size - 1)
        return remote(src, out_rows(head, 0, own_rows), far_send.at[head], far_recv.at[head], target)

    def near_copy(head):
        src = own_ref.at[pl.ds(head * own_rows, own_rows)]
        return remote(
            src, out_rows(head, 1, own_rows), near_send.at[head], near_recv.at[head], partners[0]
        )

    def relay_copy(head):
        return remote(
            out_rows(head, 0, own_rows), out_rows(head, 1, own_rows),
            near_send.at[head], near_recv.at[head], partners[0],
        )

    barrier = pltpu.get_barrier_semaphore()
    for partner in partners:
        pl.semaphore_signal(
            barrier, inc=1, device_id={"ctx": partner}, device_id_type=pl.DeviceIdType.MESH
        )

    @pl.when(sends_far)
    def _():
        pl.semaphore_signal(
            barrier, inc=1, device_id={"ctx": device + REACH}, device_id_type=pl.DeviceIdType.MESH
        )

    @pl.when(gets_far)
    def _():
        pl.semaphore_signal(
            barrier, inc=1, device_id={"ctx": device - REACH}, device_id_type=pl.DeviceIdType.MESH
        )

    arrivals = rounds + sends_far.astype(jnp.int32) + gets_far.astype(jnp.int32)
    pl.semaphore_wait(barrier, arrivals)

    def start_far(heads):
        @pl.when(sends_far)
        def _():
            for head in heads:
                far_copy(head).start()

    early = range(kv_heads // 2)
    late = range(kv_heads // 2, kv_heads)
    base = jnp.int32(0)
    length = kv_heads * col_rows
    offset = 0
    bases = []
    folds = []
    for k in range(rounds):
        half = length // 2
        kept = pl.multiple_of(base + bits[k] * half, 16)
        given = pl.multiple_of(base + (1 - bits[k]) * half, 16)
        source = term_ref if k == 0 else acc
        copy = remote(
            source.at[pl.ds(given, half)], landed.at[pl.ds(offset, half)],
            fold_send.at[k], fold_recv.at[k], partners[k],
        )
        copy.start()
        folds.append(copy)
        if k == min(1, rounds - 1):
            start_far(early)
            for head in range(kv_heads):
                pltpu.make_async_copy(
                    own_ref.at[pl.ds(head * own_rows, own_rows)],
                    out_rows(head, REACH, own_rows), keep_sem.at[head],
                ).start()

            @pl.when(odd == 0)
            def _():
                for head in range(kv_heads):
                    near_copy(head).start()

        if k == rounds - 1:
            start_far(late)
        copy.wait_recv()
        step = min(half, 256)

        def add(i, carry, kept=kept, offset=offset, source=source, step=step, k=k):
            here = pl.ds(pl.multiple_of(kept + i * step, 16), step)
            there = pl.ds(pl.multiple_of(offset + i * step, 16), step)
            total = source[here, :] + landed[there, :]
            if k == rounds - 1:
                full[here, :] = total
            else:
                acc[here, :] = total
            return carry

        lax.fori_loop(0, half // step, add, 0)
        bases.append(kept)
        base, length, offset = kept, half, offset + half

    grows = []
    for k in reversed(range(rounds)):
        part = pl.ds(bases[k], (kv_heads * col_rows) >> (k + 1))
        copy = remote(full.at[part], full.at[part], grow_send.at[k], grow_recv.at[k], partners[k])
        copy.start()
        grows.append(copy)
        copy.wait_recv()

    cols = []
    for head in range(kv_heads):
        copy = pltpu.make_async_copy(
            full.at[pl.ds(head * col_rows, col_rows)],
            out_rows(head, REACH + 1, col_rows), keep_sem.at[kv_heads + head],
        )
        copy.start()
        cols.append(copy)

    @pl.when(gets_far)
    def _():
        for head in range(kv_heads):
            far_copy(head).wait_recv()

            @pl.when(odd == 1)
            def _(head=head):
                relay_copy(head).start()

    @pl.when((odd == 1) | gets_far)
    def _():
        for head in range(kv_heads):
            near_copy(head).wait_recv()

    @pl.when((odd == 0) | gets_far)
    def _():
        for head in range(kv_heads):
            near_copy(head).wait_send()

    @pl.when(sends_far)
    def _():
        for head in range(kv_heads):
            far_copy(head).wait_send()

    for copy in folds + grows:
        copy.wait_send()
    for head in range(kv_heads):
        pltpu.make_async_copy(
            own_ref.at[pl.ds(head * own_rows, own_rows)],
            out_rows(head, REACH, own_rows), keep_sem.at[head],
        ).wait()
    for copy in cols:
        copy.wait()


def spread(own, term):
    size = lax.axis_size("ctx")
    kv_heads, per_dev, _, _, head_dim = own.shape
    n_vert = term.shape[1]
    own_rows = per_dev * 2 * BLOCK
    col_rows = n_vert * 2 * BLOCK
    n_tiles = (REACH + 1) * per_dev + n_vert
    dims = (size, kv_heads, own_rows, col_rows)
    rounds = size.bit_length() - 1
    dma = pltpu.SemaphoreType.DMA
    columns = pltpu.VMEM((kv_heads * col_rows, head_dim), own.dtype)
    out = pl.pallas_call(
        functools.partial(spread_kernel, dims),
        out_shape=jax.ShapeDtypeStruct((kv_heads * n_tiles * 2 * BLOCK, head_dim), own.dtype),
        in_specs=[pl.BlockSpec(memory_space=pltpu.VMEM)] * 2,
        out_specs=pl.BlockSpec(memory_space=pl.ANY),
        scratch_shapes=[columns, columns, columns]
        + [dma((kv_heads,))] * 4
        + [dma((rounds,))] * 4
        + [dma((2 * kv_heads,))],
        compiler_params=pltpu.CompilerParams(
            collective_id=0, has_side_effects=True, vmem_limit_bytes=48 * 1024 * 1024
        ),
        name="spread",
    )(own.reshape(-1, head_dim), term.reshape(-1, head_dim))
    return out.reshape(kv_heads, n_tiles, 2, BLOCK, head_dim)


def local(
    query_states, key_states, value_states, vert_blocks, vert_count, slash_offsets, slash_count
):
    rows_dev, q_heads, head_dim = query_states.shape
    kv_heads = key_states.shape[1]
    group_size = q_heads // kv_heads
    per_dev = rows_dev // BLOCK
    n_vert = vert_blocks.shape[1]
    device = lax.axis_index("ctx")

    def by_tile(x):
        return jnp.transpose(x.reshape(per_dev, BLOCK, kv_heads, head_dim), (2, 0, 1, 3))

    own = jnp.stack((by_tile(key_states), by_tile(value_states)), axis=2)
    local_block = vert_blocks - device * per_dev
    used_slot = jnp.arange(n_vert)[None, :] < vert_count[:, None]
    mine = used_slot & (local_block >= 0) & (local_block < per_dev)
    term = jnp.take_along_axis(
        own, jnp.clip(local_block, 0, per_dev - 1)[:, :, None, None, None], axis=1
    )
    term = jnp.where(mine[:, :, None, None, None], term, jnp.bfloat16(0))
    tiles = spread(own, term)
    out = attend(
        query_states.reshape(rows_dev, q_heads * head_dim),
        tiles,
        vert_blocks,
        vert_count,
        slash_offsets,
        slash_count,
        device.reshape(1).astype(jnp.int32),
        group_size,
    )
    return out.reshape(rows_dev, q_heads, head_dim)


def solution(mesh):
    in_specs = (
        P(("groups", "ctx"), None, None),
        P(("groups", "ctx"), None, None),
        P(("groups", "ctx"), None, None),
        P("groups", None),
        P("groups"),
        P("groups", None),
        P("groups"),
    )
    out_specs = P(("groups", "ctx"), None, None)
    return jax.shard_map(local, mesh=mesh, in_specs=in_specs, out_specs=out_specs, check_vma=False)
```
